32 devices in a mesh: fsdp: 8 (over z, core), expert: 2 (over x), dp: 2 (over y).
Axes of the slice: x: 2, y: 2, z: 4, core: 2. Of those that a mesh axis runs over, the one named last changes fastest.
Arguments:
- tokens: bfloat16 [16, 4, 2048], P('fsdp', ('expert', 'dp')), may hold values from -6 to 6
- cotangent: bfloat16 [16, 4, 2048], P('fsdp', ('expert', 'dp')), may hold values from -4 to 4
- expert_ids: int32 [16, 4, 2], P(None, ('expert', 'dp')), may hold values from 0 to 3, as said below
- slot_ids: int32 [16, 4, 2], P(None, ('expert', 'dp')), may hold values from -1 to 7, as said below
- route_probs: bfloat16 [16, 4, 2], P(None, ('expert', 'dp')), may hold values from 0.049804688 to 0.94921875
- gate_weight: bfloat16 [4, 2048, 8192], P('expert', None, 'fsdp'), may hold values from -0.125 to 0.125
- up_weight: bfloat16 [4, 2048, 8192], P('expert', None, 'fsdp'), may hold values from -0.125 to 0.125
- down_weight: bfloat16 [4, 8192, 2048], P('expert', 'fsdp'), may hold values from -0.0625 to 0.0625
Outputs:
- grad_gate: bfloat16 [4, 2048, 8192], P('expert', 'dp', 'fsdp')
- grad_up: bfloat16 [4, 2048, 8192], P('expert', 'dp', 'fsdp')
- grad_down: bfloat16 [4, 8192, 2048], P('expert', 'fsdp', 'dp')
- token_grad: bfloat16 [16, 4, 2048], P('fsdp', ('expert', 'dp'))
- prob_grad: float32 [16, 4, 2], P('fsdp', ('expert', 'dp'))
The draws below stay inside these ranges and needn't reach their ends.
Inputs may be any that keep to these rules, and one draw needn't show every extreme that they name: `expert_ids`: each token names two different experts. `slot_ids`: within a group, the choices of one expert get slots 0, 1, 2, ... by arrival in token order, a token's first choice before its second; a choice arriving after all 8 slots of its expert are taken gets -1 and is dropped. In every group some expert receives more than 8 choices, and it is the same expert in all groups of one dp index.
All inputs are finite; a program needn't handle non-finite values.
Results may differ from the reference program's by a relative error of at most 0.015.
Values may be sent and summed in bfloat16 or wider, within the bound.
A program may use at most 128 MiB of HBM per device.

```python
import jax
import jax.numpy as jnp
from jax import lax

D = 2048
FF = 8192
EXPERTS = 4
GROUP_TOKENS = 16
GROUPS = 4
CAP = 8
N_EXPERT = 2
N_DP = 2


def route_table(key):
    folded = jax.random.fold_in(key, 4099)
    subkeys = jax.random.split(folded, 4)
    hot_expert = jax.random.randint(subkeys[0], (N_DP,), 0, EXPERTS)
    group_hot = jnp.tile(hot_expert, N_EXPERT)
    token_iota = jnp.arange(GROUP_TOKENS, dtype=jnp.int32)[:, None]
    raw_rank = jax.random.randint(subkeys[1], (GROUP_TOKENS, GROUPS), 0, 1 << 16) * GROUP_TOKENS + token_iota
    position = jnp.argsort(jnp.argsort(raw_rank, axis=0, stable=True), axis=0, stable=True)
    pinned = position < GROUP_TOKENS // 2
    uniform_pick = jax.random.randint(subkeys[2], (GROUP_TOKENS, GROUPS), 0, EXPERTS)
    leading = jnp.where(pinned, group_hot[None, :], uniform_pick)
    offset = jax.random.randint(subkeys[3], (GROUP_TOKENS, GROUPS), 1, EXPERTS)
    trailing = (leading + offset) % EXPERTS
    chosen = jnp.stack([leading, trailing], axis=-1).astype(jnp.int32)
    flattened = jnp.transpose(chosen, (0, 2, 1)).reshape(GROUP_TOKENS * 2, GROUPS)
    matches = (flattened[:, :, None] == jnp.arange(EXPERTS, dtype=jnp.int32)[None, None, :]).astype(jnp.int32)
    before = jnp.cumsum(matches, axis=0) - matches
    arrival = jnp.sum(before * matches, axis=-1)
    arrival = jnp.where(arrival < CAP, arrival, -1)
    slot_table = jnp.transpose(arrival.reshape(GROUP_TOKENS, 2, GROUPS), (0, 2, 1)).astype(jnp.int32)
    return (chosen, slot_table)


def draw_expert_ids(key, part):
    return route_table(key)[0]


def draw_slot_ids(key, part):
    return route_table(key)[1]


def levels(rng, extent, cuts, low, top_value):
    def one(axis_at, blocks):
        steps = jax.random.uniform(jax.random.fold_in(jax.random.fold_in(rng, 6), axis_at), (blocks,), jnp.float32, low / len(cuts), top_value / len(cuts))
        return jnp.repeat(jnp.exp(steps), extent[axis_at] // blocks).reshape((-1,) + (1,) * (len(extent) - axis_at - 1))

    factor_of = one(*cuts[0])
    for cut in cuts[1:]:
        factor_of = factor_of * one(*cut)
    return factor_of


def gaussian(own_key, shape, spread, limit, cuts=(), held_as=jnp.bfloat16):
    array = spread * jax.random.normal(own_key, shape, jnp.float32)
    if cuts:
        array = array * levels(own_key, shape, cuts, -0.22, 0.18)
    return jnp.clip(array, -limit, limit).astype(held_as)


def setup_inputs(seed: int = 0) -> dict:
    key_list = jax.random.split(jax.random.key(seed), 9)
    return {
        "tokens": gaussian(key_list[0], (GROUP_TOKENS, GROUPS, D), 1.0, 6.0, ((0, 8), (1, 4))),
        "cotangent": gaussian(key_list[1], (GROUP_TOKENS, GROUPS, D), 0.5, 4.0, ((0, 8), (1, 4))),
        "expert_ids": draw_expert_ids(jax.random.fold_in(key_list[8], 71), 0),
        "slot_ids": draw_slot_ids(jax.random.fold_in(key_list[8], 71), 0),
        "route_probs": jnp.clip(0.049804688 + 0.89941406 * jax.random.uniform(key_list[4], (GROUP_TOKENS, GROUPS, 2), jnp.float32) ** levels(key_list[4], (GROUP_TOKENS, GROUPS, 2), ((1, 4),), -0.2, 0.2), 0.049804688, 0.94921875).astype(jnp.bfloat16),
        "gate_weight": gaussian(key_list[5], (EXPERTS, D, FF), D ** -0.5, 0.125, ((0, 2), (2, 8))),
        "up_weight": gaussian(key_list[6], (EXPERTS, D, FF), D ** -0.5, 0.125, ((0, 2), (2, 8))),
        "down_weight": gaussian(key_list[7], (EXPERTS, FF, D), FF ** -0.5, 0.0625, ((0, 2), (1, 8))),
    }


def rounded(values):
    return lax.optimization_barrier(values.astype(jnp.bfloat16)).astype(jnp.float32)


def group_dispatch(group_x, group_dy, group_ids, group_slots, group_probs):
    total_rows = EXPERTS * CAP
    kept_slot = group_slots >= 0
    target = group_ids * CAP + jnp.where(kept_slot, group_slots, 0)
    row_iota = lax.broadcasted_iota(jnp.int32, (total_rows, GROUP_TOKENS), 0)
    leading = jnp.logical_and(row_iota == target[None, :, 0], kept_slot[None, :, 0])
    trailing = jnp.logical_and(row_iota == target[None, :, 1], kept_slot[None, :, 1])
    either = jnp.logical_or(leading, trailing).astype(jnp.bfloat16)
    sent_x = jnp.dot(either, group_x, preferred_element_type=jnp.float32).astype(jnp.bfloat16)
    sent_dy = jnp.dot(either, group_dy, preferred_element_type=jnp.float32).astype(jnp.bfloat16)
    prob_pair = group_probs.astype(jnp.float32)
    sent_prob = jnp.sum(jnp.where(leading, prob_pair[None, :, 0], 0.0) + jnp.where(trailing, prob_pair[None, :, 1], 0.0), axis=1)
    return sent_x, sent_dy, sent_prob


def regroup(values):
    trailing_dims = values.shape[2:]
    sectioned = values.reshape((N_EXPERT, N_DP, EXPERTS, CAP) + trailing_dims)
    axes_order = (2, 1, 0, 3) + tuple(range(4, 4 + len(trailing_dims)))
    return jnp.transpose(sectioned, axes_order).reshape((EXPERTS, N_DP, N_EXPERT * CAP) + trailing_dims)


def ungroup(values):
    trailing_dims = values.shape[3:]
    sectioned = values.reshape((EXPERTS, N_DP, N_EXPERT, CAP) + trailing_dims)
    axes_order = (2, 1, 0, 3) + tuple(range(4, 4 + len(trailing_dims)))
    return jnp.transpose(sectioned, axes_order).reshape((GROUPS, EXPERTS * CAP) + trailing_dims)


def expert_backward(operands):
    input_rows, upstream_rows, rows_prob, gate_matrix, up_matrix, down_matrix = operands
    grad_gate = jnp.zeros((D, FF), jnp.float32)
    grad_up = jnp.zeros((D, FF), jnp.float32)
    grad_down = jnp.zeros((FF, D), jnp.float32)
    slot_grads = []
    slot_scores = []
    for replica in range(N_DP):
        rows_x = input_rows[replica]
        rows_dy = upstream_rows[replica]
        prob_column = rows_prob[replica][:, None]
        gate_value = jnp.dot(rows_x, gate_matrix, preferred_element_type=jnp.float32)
        up_value = jnp.dot(rows_x, up_matrix, preferred_element_type=jnp.float32)
        sigmoid_gate = jax.nn.sigmoid(gate_value)
        swish_gate = gate_value * sigmoid_gate
        hidden_full = swish_gate * up_value
        hidden = hidden_full.astype(jnp.bfloat16)
        scaled = (prob_column * hidden_full).astype(jnp.bfloat16)
        back_value = jnp.dot(rows_dy, down_matrix.T, preferred_element_type=jnp.float32)
        row_score = jnp.sum(hidden.astype(jnp.float32) * back_value, axis=1)
        back_scaled = prob_column * back_value
        grad_pre = (back_scaled * up_value * sigmoid_gate * (1.0 + gate_value * (1.0 - sigmoid_gate))).astype(jnp.bfloat16)
        grad_upper = (back_scaled * swish_gate).astype(jnp.bfloat16)
        grad_gate = grad_gate + rounded(jnp.dot(rows_x.T, grad_pre, preferred_element_type=jnp.float32))
        grad_up = grad_up + rounded(jnp.dot(rows_x.T, grad_upper, preferred_element_type=jnp.float32))
        grad_down = grad_down + rounded(jnp.dot(scaled.T, rows_dy, preferred_element_type=jnp.float32))
        slot_dx = jnp.dot(grad_pre, gate_matrix.T, preferred_element_type=jnp.float32) + jnp.dot(grad_upper, up_matrix.T, preferred_element_type=jnp.float32)
        slot_grads.append(slot_dx)
        slot_scores.append(row_score)
    return (grad_gate.astype(jnp.bfloat16), grad_up.astype(jnp.bfloat16), grad_down.astype(jnp.bfloat16), jnp.stack(slot_grads), jnp.stack(slot_scores))


def group_combine(group_dx, group_score, group_ids, group_slots):
    kept_slot = group_slots >= 0
    target = (group_ids * CAP + jnp.where(kept_slot, group_slots, 0)).astype(jnp.int32)
    picked = jnp.take(group_dx, target.reshape(-1), axis=0).reshape(GROUP_TOKENS, 2, D)
    token_dx = jnp.sum(jnp.where(kept_slot[:, :, None], picked, 0.0), axis=1)
    prob_grad = jnp.where(kept_slot, jnp.take(group_score, target), 0.0)
    return token_dx, prob_grad


def reference(tokens, cotangent, expert_ids, slot_ids, route_probs, gate_weight, up_weight, down_weight):
    sent_x, sent_dy, sent_prob = jax.vmap(group_dispatch, in_axes=(1, 1, 1, 1, 1))(tokens, cotangent, expert_ids, slot_ids, route_probs)
    outcome = lax.map(expert_backward, (regroup(sent_x), regroup(sent_dy), regroup(sent_prob), gate_weight, up_weight, down_weight))
    grad_gate, grad_up, grad_down, slot_dx, slot_score = outcome
    token_dx, prob_grad = jax.vmap(group_combine, in_axes=(0, 0, 1, 1), out_axes=(1, 1))(ungroup(slot_dx), ungroup(slot_score), expert_ids, slot_ids)
    return grad_gate, grad_up, grad_down, token_dx.astype(jnp.bfloat16), prob_grad
```

```python
import functools

import jax
import jax.numpy as jnp
from jax import lax
from jax.experimental import pallas as pl
from jax.experimental.pallas import tpu as pltpu
from jax.sharding import PartitionSpec as P

MESH = pl.DeviceIdType.MESH
TILE_ROWS = 16
NT = (((1,), (1,)), ((), ()))
TN = (((0,), (0,)), ((), ()))


def block_iota(shape, dim):
    return lax.broadcasted_iota(jnp.int32, shape, dim)


def exchange_kernel(
    n_fsdp, n_expert, n_dp, capacity,
    payload, meta, gate_hbm, up_hbm, down_hbm,
    half_x, half_y, pre_out, upper_out, scaled_out, dx_out, prob_out,
    gate_w, up_w, down_w, gathered, metas, rows_x, rows_y, match_ref, score_acc,
    stack, send_dx, recv_dx, send_score, recv_score,
    weight_sem, local_sem, za_send, za_recv, xb_send, xb_recv, mb_send, mb_recv,
    core_send, core_recv, dx_ssem, dx_rsem, sc_ssem, sc_rsem,
):
    f = lax.axis_index("fsdp")
    e = lax.axis_index("expert")
    r = lax.axis_index("dp")
    cores = 2
    n_z = n_fsdp // cores
    z, core = f // cores, f % cores
    groups = n_expert * n_dp
    local_experts, width, hidden_count = gate_w.shape
    quarter = payload.shape[1]
    per_rep = n_expert * capacity
    per_expert = n_dp * per_rep
    all_rows = local_experts * per_expert
    own_rows = local_experts * per_rep
    lanes = groups * n_fsdp * TILE_ROWS
    strips = TILE_ROWS // 2
    strip = width // strips

    weight_copies = []
    for k in range(local_experts):
        for at, (src, dst) in enumerate(((gate_hbm, gate_w), (up_hbm, up_w), (down_hbm, down_w))):
            copy = pltpu.make_async_copy(src.at[k], dst.at[k], weight_sem.at[k, at])
            copy.start()
            weight_copies.append(copy)

    def device(df, de, dr):
        return {"fsdp": df, "expert": de, "dp": dr}

    def zpeer(step):
        return lax.rem(z + step, n_z) * cores + core

    cross = [(a, b) for a in range(n_expert) for b in range(n_dp) if (a, b) != (0, 0)]
    back = [(a, b) for a in range(n_expert) for b in range(n_fsdp) if (a, b) != (0, 0)]

    def epeer(a):
        return lax.rem(e + a, n_expert)

    def rpeer(b):
        return lax.rem(r + b, n_dp)

    barrier = pltpu.get_barrier_semaphore()
    count = 0
    for a, b in back:
        pl.semaphore_signal(barrier, inc=1, device_id=device(lax.rem(f + b, n_fsdp), epeer(a), r), device_id_type=MESH)
        count += 1
    for a, b in cross:
        if b:
            pl.semaphore_signal(barrier, inc=1, device_id=device(f, epeer(a), rpeer(b)), device_id_type=MESH)
            count += 1

    def slot(group, at_core, at_z):
        return (group * cores + at_core) * n_z + at_z

    group = e * n_dp + r
    mine = slot(group, core, z)
    own_copy = pltpu.make_async_copy(payload, gathered.at[mine], local_sem.at[0])
    own_copy.start()
    own_meta = pltpu.make_async_copy(meta, metas.at[group], local_sem.at[1])
    own_meta.start()
    pl.semaphore_wait(barrier, count)

    sent = []
    ring = []
    for step in range(1, n_z):
        copy = pltpu.make_async_remote_copy(
            payload, gathered.at[mine], za_send.at[step], za_recv.at[step],
            device_id=device(zpeer(step), e, r), device_id_type=MESH,
        )
        copy.start()
        ring.append(copy)
    crossing = {}

    def cross_send(step):
        block = slot(group, core, lax.rem(z + n_z - step, n_z))
        src = payload if step == 0 else gathered.at[block]
        for at, (a, b) in enumerate(cross):
            copy = pltpu.make_async_remote_copy(
                src, gathered.at[block], xb_send.at[at, step], xb_recv.at[at, step],
                device_id=device(f, epeer(a), rpeer(b)), device_id_type=MESH,
            )
            copy.start()
            crossing[at, step] = copy

    meta_copies = []
    for at, (a, b) in enumerate(cross):
        copy = pltpu.make_async_remote_copy(
            meta, metas.at[group], mb_send.at[at], mb_recv.at[at],
            device_id=device(f, epeer(a), rpeer(b)), device_id_type=MESH,
        )
        copy.start()
        meta_copies.append(copy)
    cross_send(0)
    own_copy.wait()
    own_meta.wait()
    near = sorted(range(1, n_z), key=lambda s: (min(s, n_z - s), s))
    for step in near:
        ring[step - 1].wait_recv()
        cross_send(step)

    partner = device(z * cores + 1 - core, e, r)
    core_copies = []

    def core_exchange(at, which):
        slab = pl.ds(slot(which, core, 0), n_z)
        copy = pltpu.make_async_remote_copy(
            gathered.at[slab], gathered.at[slab], core_send.at[at], core_recv.at[at],
            device_id=partner, device_id_type=MESH,
        )
        copy.start()
        core_copies.append(copy)

    core_exchange(len(cross), group)

    for copy in meta_copies:
        copy.wait_recv()
    code0 = jnp.concatenate([metas[g, 0:1, :] for g in range(groups)], axis=1)
    code1 = jnp.concatenate([metas[g, 1:2, :] for g in range(groups)], axis=1)
    prob0 = jnp.concatenate([metas[g, 2:3, :] for g in range(groups)], axis=1)
    prob1 = jnp.concatenate([metas[g, 3:4, :] for g in range(groups)], axis=1)
    experts = local_experts * n_expert
    row_codes = []
    for k in range(local_experts):
        for rr in range(n_dp):
            for ee in range(n_expert):
                start = (ee * n_dp + rr) * (experts * capacity) + (e * local_experts + k) * capacity
                row_codes.append(block_iota((capacity, lanes), 0) + start)
    row_code = jnp.concatenate(row_codes, axis=0).astype(jnp.float32)
    place = lax.rem(block_iota((all_rows, lanes), 1), TILE_ROWS)
    match0 = jnp.where(row_code == code0, 1.0, 0.0)
    match1 = jnp.where(row_code == code1, 1.0, 0.0)
    match_ref[0] = match0
    match_ref[1] = match1
    first = jnp.where(place == 0, 1.0, 0.0)
    single = first + jnp.where(place == TILE_ROWS // 4, 1.0, 0.0)
    prob_rows = jnp.sum(single * (match0 * prob0 + match1 * prob1), axis=1, keepdims=True)
    both = match0 + match1
    masks = []
    for kind in range(2):
        for c in range(4):
            lo = kind * (TILE_ROWS // 2) + c
            keep = jnp.where(place == lo, 1.0, 0.0) + jnp.where(place == lo + 4, 1.0, 0.0)
            masks.append((both * keep).astype(jnp.bfloat16))

    combos = strips * own_rows
    message_rows = n_expert * n_fsdp * TILE_ROWS
    m_col = block_iota((message_rows, lanes), 0)
    m_tile = m_col // TILE_ROWS
    m_tok = (m_col // strips) % 2
    m_e = m_tile // n_fsdp
    m_f = m_tile % n_fsdp
    m_slot = ((m_e * n_dp + r) * cores + m_f % cores) * n_z + m_f // cores
    target_lane = m_slot * TILE_ROWS + m_tok * 4
    select = jnp.where(block_iota((message_rows, lanes), 1) == target_lane, 1.0, 0.0).astype(jnp.bfloat16)
    strip_keep = (
        block_iota((message_rows, combos), 0) % strips
        == block_iota((message_rows, combos), 1) // own_rows
    )
    combine = []
    for c in range(2):
        own = [
            match_ref[c, pl.ds(pl.multiple_of(k * per_expert + r * per_rep, per_rep), per_rep), :]
            for k in range(local_experts)
        ]
        tiled = jnp.concatenate(own * strips, axis=0).astype(jnp.bfloat16)
        picked = lax.dot_general(select, tiled, NT, preferred_element_type=jnp.float32)
        combine.append(jnp.where(strip_keep, picked, 0.0).astype(jnp.bfloat16))

    for at, (a, b) in enumerate(cross):
        for step in range(n_z):
            crossing[at, step].wait_recv()
        source = lax.rem(e + n_expert - a, n_expert) * n_dp + lax.rem(r + n_dp - b, n_dp)
        core_exchange(at, source)
    for copy in core_copies:
        copy.wait_recv()

    everything = gathered[...].reshape(groups * n_fsdp * TILE_ROWS, quarter)
    for c in range(4):
        span = slice(c * quarter, (c + 1) * quarter)
        rows_x[:, span] = jnp.dot(masks[c], everything, preferred_element_type=jnp.float32).astype(jnp.bfloat16)
        rows_y[:, span] = jnp.dot(masks[4 + c], everything, preferred_element_type=jnp.float32).astype(jnp.bfloat16)

    chunk = hidden_count // 2
    for k in range(local_experts):
        for copy in weight_copies[3 * k : 3 * k + 3]:
            copy.wait()
        rows = slice(k * per_expert, (k + 1) * per_expert)
        prob = prob_rows[rows]
        score_acc[rows, :] = jnp.zeros((per_expert, 128), jnp.float32)
        for part in range(hidden_count // chunk):
            cols = slice(part * chunk, (part + 1) * chunk)
            x = rows_x[rows, :]
            gate_value = jnp.dot(x, gate_w[k, :, cols], preferred_element_type=jnp.float32)
            up_value = jnp.dot(x, up_w[k, :, cols], preferred_element_type=jnp.float32)
            back_value = lax.dot_general(
                rows_y[rows, :], down_w[k, cols, :], NT, preferred_element_type=jnp.float32
            )
            sigmoid_gate = jax.nn.sigmoid(gate_value)
            swish_gate = gate_value * sigmoid_gate
            hidden_full = swish_gate * up_value
            score = hidden_full.astype(jnp.bfloat16).astype(jnp.float32) * back_value
            total = score[:, :128]
            for at in range(128, chunk, 128):
                total = total + score[:, at : at + 128]
            score_acc[rows, :] += total
            back_scaled = prob * back_value
            scaled_out[rows, cols] = (prob * hidden_full).astype(jnp.bfloat16)
            pre_out[rows, cols] = (
                back_scaled * up_value * sigmoid_gate * (1.0 + gate_value * (1.0 - sigmoid_gate))
            ).astype(jnp.bfloat16)
            upper_out[rows, cols] = (back_scaled * swish_gate).astype(jnp.bfloat16)

    def return_all(src, dst, ssem, rsem):
        copies = []
        for at, (a, b) in enumerate(back):
            to_e, to_f = epeer(a), lax.rem(f + b, n_fsdp)
            spot = pl.multiple_of((to_e * n_fsdp + to_f) * TILE_ROWS, TILE_ROWS)
            copy = pltpu.make_async_remote_copy(
                src.at[pl.ds(spot, TILE_ROWS)], dst.at[at], ssem.at[at], rsem.at[at],
                device_id=device(to_f, to_e, r), device_id_type=MESH,
            )
            copy.start()
            copies.append(copy)
        return copies

    own_at = [
        pl.ds(pl.multiple_of(k * per_expert + r * per_rep, per_rep), per_rep)
        for k in range(local_experts)
    ]
    own_score = jnp.concatenate([score_acc[at, :] for at in own_at] * strips, axis=0)
    own_score = jnp.sum(own_score, axis=1, keepdims=True)
    wide = jnp.broadcast_to(own_score, (combos, 128)).astype(jnp.bfloat16)
    lead = jnp.dot(combine[0], wide, preferred_element_type=jnp.float32)
    trail = jnp.dot(combine[1], wide, preferred_element_type=jnp.float32)
    lane = block_iota((message_rows, 128), 1)
    send_score[...] = jnp.where(lane == 0, lead, jnp.where(lane == 1, trail, 0.0)).astype(jnp.bfloat16)
    score_copies = return_all(send_score, recv_score, sc_ssem, sc_rsem)

    for k in range(local_experts):
        pre = pre_out[own_at[k], :]
        upper = upper_out[own_at[k], :]
        for s in range(strips):
            feats = slice(s * strip, (s + 1) * strip)
            value = lax.dot_general(pre, gate_w[k, feats, :], NT, preferred_element_type=jnp.float32)
            value += lax.dot_general(upper, up_w[k, feats, :], NT, preferred_element_type=jnp.float32)
            base = s * own_rows + k * per_rep
            stack[base : base + per_rep, :] = value.astype(jnp.bfloat16)
    send_dx[...] = jnp.dot(
        combine[0] + combine[1], stack[...], preferred_element_type=jnp.float32
    ).astype(jnp.bfloat16)
    dx_copies = return_all(send_dx, recv_dx, dx_ssem, dx_rsem)

    half = half_x.shape[1]
    mid = pl.ds(pl.multiple_of(r * half, half), half)
    half_x[...] = rows_x[:, mid]
    half_y[...] = rows_y[:, mid]

    own_spot = pl.ds(pl.multiple_of((e * n_fsdp + f) * TILE_ROWS, TILE_ROWS), TILE_ROWS)
    total = send_score[own_spot, :].astype(jnp.float32)
    for at, copy in enumerate(score_copies):
        copy.wait_recv()
        total = total + recv_score[at].astype(jnp.float32)
    prob_out[...] = total
    total = send_dx[own_spot, :].astype(jnp.float32)
    for at, copy in enumerate(dx_copies):
        copy.wait_recv()
        total = total + recv_dx[at].astype(jnp.float32)
    dx_out[...] = total.astype(jnp.bfloat16)
    for copy in ring + list(crossing.values()) + meta_copies + core_copies + score_copies + dx_copies:
        copy.wait_send()


def weight_kernel(x_ref, y_ref, pre_ref, upper_ref, scaled_ref, gate_ref, up_ref, down_ref):
    x = x_ref[...]
    gate_ref[0] = lax.dot_general(x, pre_ref[...], TN, preferred_element_type=jnp.float32).astype(jnp.bfloat16)
    up_ref[0] = lax.dot_general(x, upper_ref[...], TN, preferred_element_type=jnp.float32).astype(jnp.bfloat16)
    down_ref[0] = lax.dot_general(scaled_ref[...], y_ref[...], TN, preferred_element_type=jnp.float32).astype(jnp.bfloat16)


def fits(tokens, expert_ids, gate_weight):
    n_fsdp, n_expert, n_dp = (lax.axis_size(a) for a in ("fsdp", "expert", "dp"))
    group_count = expert_ids.shape[0]
    experts = gate_weight.shape[0] * n_expert
    capacity = 2 * group_count // experts
    width, hidden = gate_weight.shape[1:]
    weights = 3 * gate_weight.size * 2
    return (
        tokens.shape[0] == 2
        and n_fsdp % 2 == 0
        and n_fsdp * TILE_ROWS % 128 == 0
        and capacity % 8 == 0
        and n_expert * capacity % 16 == 0
        and n_expert * n_dp * n_fsdp * TILE_ROWS <= 1024
        and gate_weight.shape[0] * n_expert * capacity * n_dp <= 128
        and width % (128 * n_dp) == 0
        and width % 1024 == 0
        and hidden % 256 == 0
        and weights <= 32 * 1024 * 1024
    )


def fused(tokens, cotangent, expert_ids, slot_ids, route_probs, gate_weight, up_weight, down_weight):
    n_fsdp, n_expert, n_dp = (lax.axis_size(a) for a in ("fsdp", "expert", "dp"))
    local_experts, width, hidden = gate_weight.shape
    experts = local_experts * n_expert
    group_count = expert_ids.shape[0]
    capacity = 2 * group_count // experts
    groups = n_expert * n_dp
    cores, n_z = 2, n_fsdp // 2
    quarter = width // 4
    payload = jnp.concatenate([tokens[:, 0, :], cotangent[:, 0, :]], axis=0).reshape(TILE_ROWS, quarter)
    group = lax.axis_index("expert") * n_dp + lax.axis_index("dp")
    ids, slots = expert_ids[:, 0, :], slot_ids[:, 0, :]
    code = jnp.where(slots >= 0, group * (experts * capacity) + ids * capacity + slots, -1)
    values = jnp.concatenate([code.astype(jnp.float32), route_probs[:, 0, :].astype(jnp.float32)], axis=1)
    lane = jnp.arange(n_fsdp * TILE_ROWS)
    block = lane // TILE_ROWS
    token = ((block % n_z) * cores + block // n_z) * 2 + (lane % TILE_ROWS) // 4 % 2
    hit = token[None, None, :] == jnp.arange(group_count)[:, None, None]
    meta = jnp.sum(jnp.where(hit, values[:, :, None], 0.0), axis=0)
    meta = jnp.pad(meta, ((0, 4), (0, 0)))

    per_rep = n_expert * capacity
    per_expert = n_dp * per_rep
    all_rows = local_experts * per_expert
    own_rows = local_experts * per_rep
    half = width // n_dp
    strips = TILE_ROWS // 2
    strip = width // strips
    back = n_expert * n_fsdp - 1
    cross = groups - 1
    message_rows = n_expert * n_fsdp * TILE_ROWS
    bf16, f32 = jnp.bfloat16, jnp.float32
    dma = pltpu.SemaphoreType.DMA
    vmem = pl.BlockSpec(memory_space=pltpu.VMEM)
    hbm = pl.BlockSpec(memory_space=pl.ANY)
    shape = jax.ShapeDtypeStruct
    half_x, half_y, pre, upper, scaled, dx, prob = pl.pallas_call(
        functools.partial(exchange_kernel, n_fsdp, n_expert, n_dp, capacity),
        out_shape=[
            shape((all_rows, half), bf16),
            shape((all_rows, half), bf16),
            shape((all_rows, hidden), bf16),
            shape((all_rows, hidden), bf16),
            shape((all_rows, hidden), bf16),
            shape((TILE_ROWS, strip), bf16),
            shape((TILE_ROWS, 128), f32),
        ],
        in_specs=[vmem, vmem, hbm, hbm, hbm],
        out_specs=[vmem] * 7,
        scratch_shapes=[
            pltpu.VMEM((local_experts, width, hidden), bf16),
            pltpu.VMEM((local_experts, width, hidden), bf16),
            pltpu.VMEM((local_experts, hidden, width), bf16),
            pltpu.VMEM((groups * n_fsdp, TILE_ROWS, quarter), bf16),
            pltpu.VMEM((groups, 8, n_fsdp * TILE_ROWS), f32),
            pltpu.VMEM((all_rows, width), bf16),
            pltpu.VMEM((all_rows, width), bf16),
            pltpu.VMEM((2, all_rows, groups * n_fsdp * TILE_ROWS), f32),
            pltpu.VMEM((all_rows, 128), f32),
            pltpu.VMEM((strips * own_rows, strip), bf16),
            pltpu.VMEM((message_rows, strip), bf16),
            pltpu.VMEM((back, TILE_ROWS, strip), bf16),
            pltpu.VMEM((message_rows, 128), bf16),
            pltpu.VMEM((back, TILE_ROWS, 128), bf16),
            dma((local_experts, 3)),
            dma((2,)),
            dma((n_z,)),
            dma((n_z,)),
            dma((cross, n_z)),
            dma((cross, n_z)),
            dma((cross,)),
            dma((cross,)),
            dma((groups,)),
            dma((groups,)),
            dma((back,)),
            dma((back,)),
            dma((back,)),
            dma((back,)),
        ],
        compiler_params=pltpu.CompilerParams(
            collective_id=0, has_side_effects=True, vmem_limit_bytes=56 * 1024 * 1024
        ),
    )(payload, meta, gate_weight, up_weight, down_weight)

    tile = 256
    steps = half // tile
    row_block = pl.BlockSpec((per_expert, tile), lambda k, i: (k, i))
    full_hidden = pl.BlockSpec((per_expert, hidden), lambda k, i: (k, 0))
    hidden_tile = hidden // steps
    grad_gate, grad_up, grad_down = pl.pallas_call(
        weight_kernel,
        grid=(local_experts, steps),
        out_shape=[
            shape((local_experts, half, hidden), bf16),
            shape((local_experts, half, hidden), bf16),
            shape((local_experts, hidden, half), bf16),
        ],
        in_specs=[
            row_block,
            pl.BlockSpec((per_expert, half), lambda k, i: (k, 0)),
            full_hidden,
            full_hidden,
            pl.BlockSpec((per_expert, hidden_tile), lambda k, i: (k, i)),
        ],
        out_specs=[
            pl.BlockSpec((1, tile, hidden), lambda k, i: (k, i, 0)),
            pl.BlockSpec((1, tile, hidden), lambda k, i: (k, i, 0)),
            pl.BlockSpec((1, hidden_tile, half), lambda k, i: (k, i, 0)),
        ],
        compiler_params=pltpu.CompilerParams(
            dimension_semantics=("arbitrary", "arbitrary"), vmem_limit_bytes=40 * 1024 * 1024
        ),
    )(half_x, half_y, pre, upper, scaled)
    token_grad = dx.reshape(2, 1, width)
    prob_grad = prob.reshape(2, strips, 128)[:, :1, :2]
    return grad_gate, grad_up, grad_down, token_grad, prob_grad


def either_way(tokens, cotangent, expert_ids, slot_ids, route_probs, gate_weight, up_weight, down_weight):
    way = fused if fits(tokens, expert_ids, gate_weight) else shards
    return way(tokens, cotangent, expert_ids, slot_ids, route_probs, gate_weight, up_weight, down_weight)


def route_rows(group_ids, group_slots, local_count, peer_count, capacity):
    kept_slot = group_slots >= 0
    target = (
        group_ids % local_count * (peer_count * capacity)
        + group_ids // local_count * capacity
        + jnp.where(kept_slot, group_slots, 0)
    )
    total_rows = local_count * peer_count * capacity
    row_iota = lax.broadcasted_iota(jnp.int32, (total_rows, group_ids.shape[0]), 0)
    leading = jnp.logical_and(row_iota == target[None, :, 0], kept_slot[None, :, 0])
    trailing = jnp.logical_and(row_iota == target[None, :, 1], kept_slot[None, :, 1])
    return (leading, trailing)


def summed(values):
    return jnp.sum(
        lax.optimization_barrier(values.astype(jnp.bfloat16)).astype(jnp.float32), axis=1
    )


def shards(
    tokens, cotangent, expert_ids, slot_ids, route_probs, gate_weight, up_weight, down_weight
):
    local_experts = gate_weight.shape[0]
    model_width = tokens.shape[2]
    group_count = expert_ids.shape[0]
    peer_count = lax.axis_size("expert")
    capacity = 2 * group_count // (local_experts * peer_count)
    per_expert = peer_count * capacity
    total_rows = local_experts * per_expert
    leading, trailing = route_rows(
        expert_ids[:, 0, :], slot_ids[:, 0, :], local_experts, peer_count, capacity
    )
    either = jnp.logical_or(leading, trailing).astype(jnp.bfloat16)
    prob_pair = route_probs[:, 0, :].astype(jnp.float32)
    prob_rows = jnp.sum(
        jnp.where(leading, prob_pair[None, :, 0], 0.0)
        + jnp.where(trailing, prob_pair[None, :, 1], 0.0),
        axis=1,
    )
    prob_rows = prob_rows.astype(jnp.bfloat16).reshape(local_experts, peer_count, capacity)
    own_x = tokens[:, 0, :]
    own_dy = cotangent[:, 0, :]
    group_x, group_dy = (
        lax.all_gather(own_x, "fsdp", axis=0, tiled=True),
        lax.all_gather(own_dy, "fsdp", axis=0, tiled=True),
    )
    sent_x = (
        jnp.dot(either, group_x, preferred_element_type=jnp.float32)
        .astype(jnp.bfloat16)
        .reshape(local_experts, peer_count, capacity, model_width)
    )
    sent_dy = (
        jnp.dot(either, group_dy, preferred_element_type=jnp.float32)
        .astype(jnp.bfloat16)
        .reshape(local_experts, peer_count, capacity, model_width)
    )
    recv_x, recv_dy, recv_prob = (
        lax.all_to_all(sent_x, "expert", split_axis=1, concat_axis=1, tiled=True),
        lax.all_to_all(sent_dy, "expert", split_axis=1, concat_axis=1, tiled=True),
        lax.all_to_all(prob_rows, "expert", split_axis=1, concat_axis=1, tiled=True),
    )
    rows_x = recv_x.reshape(local_experts, per_expert, model_width)
    rows_dy = recv_dy.reshape(local_experts, per_expert, model_width)
    prob_column = recv_prob.reshape(local_experts, per_expert, 1).astype(jnp.float32)
    gate_value = jnp.einsum("erd,edh->erh", rows_x, gate_weight, preferred_element_type=jnp.float32)
    up_value = jnp.einsum("erd,edh->erh", rows_x, up_weight, preferred_element_type=jnp.float32)
    back_value = jnp.einsum(
        "erd,ehd->erh", rows_dy, down_weight, preferred_element_type=jnp.float32
    )
    sigmoid_gate = jax.nn.sigmoid(gate_value)
    swish_gate = gate_value * sigmoid_gate
    hidden_full = swish_gate * up_value
    hidden = hidden_full.astype(jnp.bfloat16)
    scaled = (prob_column * hidden_full).astype(jnp.bfloat16)
    row_score = jnp.sum(hidden.astype(jnp.float32) * back_value, axis=2)
    back_scaled = prob_column * back_value
    grad_pre = (
        back_scaled * up_value * sigmoid_gate * (1.0 + gate_value * (1.0 - sigmoid_gate))
    ).astype(jnp.bfloat16)
    grad_upper = (back_scaled * swish_gate).astype(jnp.bfloat16)
    slot_dx = jnp.einsum(
        "erh,edh->erd", grad_pre, gate_weight, preferred_element_type=jnp.float32
    ) + jnp.einsum("erh,edh->erd", grad_upper, up_weight, preferred_element_type=jnp.float32)
    replica_count = lax.axis_size("dp")
    far_x, far_dy = (
        lax.all_to_all(rows_x, "dp", split_axis=2, concat_axis=1, tiled=True),
        lax.all_to_all(rows_dy, "dp", split_axis=2, concat_axis=1, tiled=True),
    )
    far_pre, far_upper, far_scaled = (
        lax.all_gather(grad_pre, "dp", axis=1, tiled=True),
        lax.all_gather(grad_upper, "dp", axis=1, tiled=True),
        lax.all_gather(scaled, "dp", axis=1, tiled=True),
    )
    quarter = far_x.shape[2]
    hidden_count = far_pre.shape[2]
    far_x = far_x.reshape(local_experts, replica_count, per_expert, quarter)
    far_dy = far_dy.reshape(local_experts, replica_count, per_expert, quarter)
    far_pre = far_pre.reshape(local_experts, replica_count, per_expert, hidden_count)
    far_upper = far_upper.reshape(local_experts, replica_count, per_expert, hidden_count)
    far_scaled = far_scaled.reshape(local_experts, replica_count, per_expert, hidden_count)
    grad_gate = summed(
        jnp.einsum("esrd,esrh->esdh", far_x, far_pre, preferred_element_type=jnp.float32)
    )
    grad_up = summed(
        jnp.einsum("esrd,esrh->esdh", far_x, far_upper, preferred_element_type=jnp.float32)
    )
    grad_down = summed(
        jnp.einsum("esrh,esrd->eshd", far_scaled, far_dy, preferred_element_type=jnp.float32)
    )
    back_dx, back_score = (
        lax.all_to_all(
            slot_dx.reshape(local_experts, peer_count, capacity, model_width).astype(jnp.bfloat16),
            "expert",
            split_axis=1,
            concat_axis=1,
            tiled=True,
        ).astype(jnp.float32),
        lax.all_to_all(
            row_score.reshape(local_experts, peer_count, capacity).astype(jnp.bfloat16),
            "expert",
            split_axis=1,
            concat_axis=1,
            tiled=True,
        ).astype(jnp.float32),
    )
    flat_dx = back_dx.reshape(total_rows, model_width)
    flat_score = back_score.reshape(total_rows)
    leading_f = leading.astype(jnp.float32)
    trailing_f = trailing.astype(jnp.float32)
    group_dx = lax.dot_general(
        leading_f + trailing_f, flat_dx, (((0,), (0,)), ((), ())), precision=lax.Precision.HIGHEST
    )
    group_prob = jnp.stack(
        [
            jnp.dot(flat_score, leading_f, precision=lax.Precision.HIGHEST),
            jnp.dot(flat_score, trailing_f, precision=lax.Precision.HIGHEST),
        ],
        axis=1,
    )
    token_dx, token_prob = (
        lax.psum_scatter(group_dx, "fsdp", scatter_dimension=0, tiled=True),
        lax.psum_scatter(group_prob, "fsdp", scatter_dimension=0, tiled=True),
    )
    return (
        grad_gate.astype(jnp.bfloat16),
        grad_up.astype(jnp.bfloat16),
        grad_down.astype(jnp.bfloat16),
        token_dx.astype(jnp.bfloat16)[:, None, :],
        token_prob[:, None, :],
    )


def solution(mesh):
    return jax.shard_map(
        either_way,
        mesh=mesh,
        in_specs=(
            P("fsdp", ("expert", "dp"), None),
            P("fsdp", ("expert", "dp"), None),
            P(None, ("expert", "dp"), None),
            P(None, ("expert", "dp"), None),
            P(None, ("expert", "dp"), None),
            P("expert", None, "fsdp"),
            P("expert", None, "fsdp"),
            P("expert", "fsdp", None),
        ),
        out_specs=(
            P("expert", "dp", "fsdp"),
            P("expert", "dp", "fsdp"),
            P("expert", "fsdp", "dp"),
            P("fsdp", ("expert", "dp"), None),
            P("fsdp", ("expert", "dp"), None),
        ),
        check_vma=False,
    )
```

```python
import functools

import jax
import jax.numpy as jnp
from jax import lax
from jax.experimental import pallas as pl
from jax.experimental.pallas import tpu as pltpu
from jax.sharding import PartitionSpec as P

MESH = pl.DeviceIdType.MESH
TILE_ROWS = 16
NT = (((1,), (1,)), ((), ()))
TN = (((0,), (0,)), ((), ()))


def block_iota(shape, dim):
    return lax.broadcasted_iota(jnp.int32, shape, dim)


def exchange_kernel(
    n_fsdp, n_expert, n_dp, capacity,
    tokens, cotangent, ids, slots, probs, gate_hbm, up_hbm, down_hbm,
    half_x, half_y, pre_out, upper_out, scaled_out, dx_out, prob_out,
    wide_payload, payload, values, meta, dx_sum,
    gate_w, up_w, down_w, gathered, metas, rows_x, rows_y, match_ref, score_acc,
    stack, send_dx, recv_dx, send_score, recv_score,
    weight_sem, local_sem, za_send, za_recv, xb_send, xb_recv, mb_send, mb_recv,
    core_send, core_recv, dx_ssem, dx_rsem, sc_ssem, sc_rsem,
):
    f = lax.axis_index("fsdp")
    e = lax.axis_index("expert")
    r = lax.axis_index("dp")
    cores = 2
    n_z = n_fsdp // cores
    z, core = f // cores, f % cores
    groups = n_expert * n_dp
    local_experts, width, hidden_count = gate_w.shape
    quarter = payload.shape[1]
    per_rep = n_expert * capacity
    per_expert = n_dp * per_rep
    all_rows = local_experts * per_expert
    own_rows = local_experts * per_rep
    lanes = groups * n_fsdp * TILE_ROWS
    strips = TILE_ROWS // 2
    strip = width // strips

    weight_copies = []
    for k in range(local_experts):
        for at, (src, dst) in enumerate(((gate_hbm, gate_w), (up_hbm, up_w), (down_hbm, down_w))):
            copy = pltpu.make_async_copy(src.at[k], dst.at[k], weight_sem.at[k, at])
            copy.start()
            weight_copies.append(copy)

    def device(df, de, dr):
        return {"fsdp": df, "expert": de, "dp": dr}

    def zpeer(step):
        return lax.rem(z + step, n_z) * cores + core

    cross = [(a, b) for a in range(n_expert) for b in range(n_dp) if (a, b) != (0, 0)]
    back = [(a, b) for a in range(n_expert) for b in range(n_fsdp) if (a, b) != (0, 0)]

    def epeer(a):
        return lax.rem(e + a, n_expert)

    def rpeer(b):
        return lax.rem(r + b, n_dp)

    barrier = pltpu.get_barrier_semaphore()
    count = 0
    for a, b in back:
        pl.semaphore_signal(barrier, inc=1, device_id=device(lax.rem(f + b, n_fsdp), epeer(a), r), device_id_type=MESH)
        count += 1
    for a, b in cross:
        if b:
            pl.semaphore_signal(barrier, inc=1, device_id=device(f, epeer(a), rpeer(b)), device_id_type=MESH)
            count += 1

    for kind, ref in enumerate((tokens, cotangent)):
        for c in range(4):
            base = kind * 8 + c * 2
            wide_payload[base : base + 2, :] = ref[:, c * quarter : (c + 1) * quarter].astype(jnp.float32)
    payload[...] = wide_payload[...].astype(jnp.bfloat16)
    group = e * n_dp + r
    experts = local_experts * n_expert
    count_tokens = ids.shape[1]
    values[...] = jnp.zeros_like(values)
    code = jnp.where(slots[...] >= 0, group * (experts * capacity) + ids[...] * capacity + slots[...], -1)
    values[0:2, 0:count_tokens] = code.astype(jnp.float32)
    values[2:4, 0:count_tokens] = probs[...].astype(jnp.float32)
    spread_lane = block_iota((128, n_fsdp * TILE_ROWS), 1)
    spread_block = spread_lane // TILE_ROWS
    spread_token = (spread_block % n_z * cores + spread_block // n_z) * 2 + spread_lane % 2
    spread = jnp.where(block_iota((128, n_fsdp * TILE_ROWS), 0) == spread_token, 1.0, 0.0)
    meta[...] = jnp.dot(
        values[...], spread, preferred_element_type=jnp.float32, precision=lax.Precision.HIGHEST
    )

    def slot(group, at_core, at_z):
        return (group * cores + at_core) * n_z + at_z

    mine = slot(group, core, z)
    own_copy = pltpu.make_async_copy(payload, gathered.at[mine], local_sem.at[0])
    own_copy.start()
    own_meta = pltpu.make_async_copy(meta, metas.at[group], local_sem.at[1])
    own_meta.start()
    pl.semaphore_wait(barrier, count)

    sent = []
    ring = []
    for step in range(1, n_z):
        copy = pltpu.make_async_remote_copy(
            payload, gathered.at[mine], za_send.at[step], za_recv.at[step],
            device_id=device(zpeer(step), e, r), device_id_type=MESH,
        )
        copy.start()
        ring.append(copy)
    crossing = {}

    def cross_send(step):
        block = slot(group, core, lax.rem(z + n_z - step, n_z))
        src = payload if step == 0 else gathered.at[block]
        for at, (a, b) in enumerate(cross):
            copy = pltpu.make_async_remote_copy(
                src, gathered.at[block], xb_send.at[at, step], xb_recv.at[at, step],
                device_id=device(f, epeer(a), rpeer(b)), device_id_type=MESH,
            )
            copy.start()
            crossing[at, step] = copy

    meta_copies = []
    for at, (a, b) in enumerate(cross):
        copy = pltpu.make_async_remote_copy(
            meta, metas.at[group], mb_send.at[at], mb_recv.at[at],
            device_id=device(f, epeer(a), rpeer(b)), device_id_type=MESH,
        )
        copy.start()
        meta_copies.append(copy)
    cross_send(0)
    own_copy.wait()
    own_meta.wait()
    near = sorted(range(1, n_z), key=lambda s: (min(s, n_z - s), s))
    for step in near:
        ring[step - 1].wait_recv()
        cross_send(step)

    partner = device(z * cores + 1 - core, e, r)
    core_copies = []

    def core_exchange(at, which):
        slab = pl.ds(slot(which, core, 0), n_z)
        copy = pltpu.make_async_remote_copy(
            gathered.at[slab], gathered.at[slab], core_send.at[at], core_recv.at[at],
            device_id=partner, device_id_type=MESH,
        )
        copy.start()
        core_copies.append(copy)

    core_exchange(len(cross), group)

    for copy in meta_copies:
        copy.wait_recv()
    code0 = jnp.concatenate([metas[g, 0:1, :] for g in range(groups)], axis=1)
    code1 = jnp.concatenate([metas[g, 1:2, :] for g in range(groups)], axis=1)
    prob0 = jnp.concatenate([metas[g, 2:3, :] for g in range(groups)], axis=1)
    prob1 = jnp.concatenate([metas[g, 3:4, :] for g in range(groups)], axis=1)
    row_codes = []
    for k in range(local_experts):
        for rr in range(n_dp):
            for ee in range(n_expert):
                start = (ee * n_dp + rr) * (experts * capacity) + (e * local_experts + k) * capacity
                row_codes.append(block_iota((capacity, lanes), 0) + start)
    row_code = jnp.concatenate(row_codes, axis=0).astype(jnp.float32)
    place = lax.rem(block_iota((all_rows, lanes), 1), TILE_ROWS)
    match0 = jnp.where(row_code == code0, 1.0, 0.0)
    match1 = jnp.where(row_code == code1, 1.0, 0.0)
    match_ref[0] = match0
    match_ref[1] = match1
    first = jnp.where(place == 0, 1.0, 0.0)
    single = first + jnp.where(place == 1, 1.0, 0.0)
    prob_rows = jnp.sum(single * (match0 * prob0 + match1 * prob1), axis=1, keepdims=True)
    both = match0 + match1
    masks = []
    for kind in range(2):
        for c in range(4):
            lo = kind * (TILE_ROWS // 2) + c * 2
            keep = jnp.where(place == lo, 1.0, 0.0) + jnp.where(place == lo + 1, 1.0, 0.0)
            masks.append((both * keep).astype(jnp.bfloat16))

    combos = strips * own_rows
    message_rows = n_expert * n_fsdp * TILE_ROWS
    m_col = block_iota((message_rows, lanes), 0)
    m_tile = m_col // TILE_ROWS
    m_tok = m_col % 2
    m_e = m_tile // n_fsdp
    m_f = m_tile % n_fsdp
    m_slot = ((m_e * n_dp + r) * cores + m_f % cores) * n_z + m_f // cores
    target_lane = m_slot * TILE_ROWS + m_tok
    select = jnp.where(block_iota((message_rows, lanes), 1) == target_lane, 1.0, 0.0).astype(jnp.bfloat16)
    strip_keep = (
        block_iota((message_rows, combos), 0) % TILE_ROWS // 2
        == block_iota((message_rows, combos), 1) // own_rows
    )
    combine = []
    for c in range(2):
        own = [
            match_ref[c, pl.ds(pl.multiple_of(k * per_expert + r * per_rep, per_rep), per_rep), :]
            for k in range(local_experts)
        ]
        tiled = jnp.concatenate(own * strips, axis=0).astype(jnp.bfloat16)
        picked = lax.dot_general(select, tiled, NT, preferred_element_type=jnp.float32)
        combine.append(jnp.where(strip_keep, picked, 0.0).astype(jnp.bfloat16))

    for at, (a, b) in enumerate(cross):
        for step in range(n_z):
            crossing[at, step].wait_recv()
        source = lax.rem(e + n_expert - a, n_expert) * n_dp + lax.rem(r + n_dp - b, n_dp)
        core_exchange(at, source)
    for copy in core_copies:
        copy.wait_recv()

    everything = gathered[...].reshape(groups * n_fsdp * TILE_ROWS, quarter)
    for c in range(4):
        span = slice(c * quarter, (c + 1) * quarter)
        rows_x[:, span] = jnp.dot(masks[c], everything, preferred_element_type=jnp.float32).astype(jnp.bfloat16)
        rows_y[:, span] = jnp.dot(masks[4 + c], everything, preferred_element_type=jnp.float32).astype(jnp.bfloat16)

    chunk = hidden_count // 2
    for k in range(local_experts):
        for copy in weight_copies[3 * k : 3 * k + 3]:
            copy.wait()
        rows = slice(k * per_expert, (k + 1) * per_expert)
        prob = prob_rows[rows]
        y = rows_y[rows, :]
        y = jnp.concatenate([y, jnp.zeros((128 - per_expert, width), jnp.bfloat16)], axis=0)
        score_acc[rows, :] = jnp.zeros((per_expert, 128), jnp.float32)
        for part in range(hidden_count // chunk):
            cols = slice(part * chunk, (part + 1) * chunk)
            x = rows_x[rows, :]
            gate_value = jnp.dot(x, gate_w[k, :, cols], preferred_element_type=jnp.float32)
            up_value = jnp.dot(x, up_w[k, :, cols], preferred_element_type=jnp.float32)
            back_value = lax.dot_general(
                down_w[k, cols, :], y, NT, preferred_element_type=jnp.float32
            ).T[:per_expert]
            sigmoid_gate = jax.nn.sigmoid(gate_value)
            swish_gate = gate_value * sigmoid_gate
            hidden_full = swish_gate * up_value
            score = hidden_full.astype(jnp.bfloat16).astype(jnp.float32) * back_value
            total = score[:, :128]
            for at in range(128, chunk, 128):
                total = total + score[:, at : at + 128]
            score_acc[rows, :] += total
            back_scaled = prob * back_value
            scaled_out[rows, cols] = (prob * hidden_full).astype(jnp.bfloat16)
            pre_out[rows, cols] = (
                back_scaled * up_value * sigmoid_gate * (1.0 + gate_value * (1.0 - sigmoid_gate))
            ).astype(jnp.bfloat16)
            upper_out[rows, cols] = (back_scaled * swish_gate).astype(jnp.bfloat16)

    def return_all(src, dst, ssem, rsem):
        copies = []
        for at, (a, b) in enumerate(back):
            to_e, to_f = epeer(a), lax.rem(f + b, n_fsdp)
            spot = pl.multiple_of((to_e * n_fsdp + to_f) * TILE_ROWS, TILE_ROWS)
            copy = pltpu.make_async_remote_copy(
                src.at[pl.ds(spot, TILE_ROWS)], dst.at[at], ssem.at[at], rsem.at[at],
                device_id=device(to_f, to_e, r), device_id_type=MESH,
            )
            copy.start()
            copies.append(copy)
        return copies

    own_at = [
        pl.ds(pl.multiple_of(k * per_expert + r * per_rep, per_rep), per_rep)
        for k in range(local_experts)
    ]
    own_score = jnp.concatenate([score_acc[at, :] for at in own_at] * strips, axis=0)
    own_score = jnp.sum(own_score, axis=1, keepdims=True)
    wide = jnp.broadcast_to(own_score, (combos, 128)).astype(jnp.bfloat16)
    lead = jnp.dot(combine[0], wide, preferred_element_type=jnp.float32)
    trail = jnp.dot(combine[1], wide, preferred_element_type=jnp.float32)
    lane = block_iota((message_rows, 128), 1)
    send_score[...] = jnp.where(lane == 0, lead, jnp.where(lane == 1, trail, 0.0)).astype(jnp.bfloat16)
    score_copies = return_all(send_score, recv_score, sc_ssem, sc_rsem)

    for k in range(local_experts):
        pre = pre_out[own_at[k], :]
        upper = upper_out[own_at[k], :]
        blank = jnp.zeros((128 - per_rep, hidden_count), jnp.bfloat16)
        pre = jnp.concatenate([pre, blank], axis=0)
        upper = jnp.concatenate([upper, blank], axis=0)
        span = 4 * strip
        for part in range(width // span):
            feats = slice(part * span, (part + 1) * span)
            value = lax.dot_general(gate_w[k, feats, :], pre, NT, preferred_element_type=jnp.float32)
            value += lax.dot_general(up_w[k, feats, :], upper, NT, preferred_element_type=jnp.float32)
            value = value.T[:per_rep].astype(jnp.bfloat16)
            for at in range(4):
                base = (part * 4 + at) * own_rows + k * per_rep
                stack[base : base + per_rep, :] = value[:, at * strip : (at + 1) * strip]
    send_dx[...] = jnp.dot(
        combine[0] + combine[1], stack[...], preferred_element_type=jnp.float32
    ).astype(jnp.bfloat16)
    dx_copies = return_all(send_dx, recv_dx, dx_ssem, dx_rsem)

    half = half_x.shape[1]
    mid = pl.ds(pl.multiple_of(r * half, half), half)
    half_x[...] = rows_x[:, mid]
    half_y[...] = rows_y[:, mid]

    own_spot = pl.ds(pl.multiple_of((e * n_fsdp + f) * TILE_ROWS, TILE_ROWS), TILE_ROWS)
    total = send_score[own_spot, :].astype(jnp.float32)
    for at, copy in enumerate(score_copies):
        copy.wait_recv()
        total = total + recv_score[at].astype(jnp.float32)
    prob_out[0] = total[0:1, 0:2]
    prob_out[1] = total[1:2, 0:2]
    total = send_dx[own_spot, :].astype(jnp.float32)
    for at, copy in enumerate(dx_copies):
        copy.wait_recv()
        total = total + recv_dx[at].astype(jnp.float32)
    dx_sum[...] = total
    for s in range(strips):
        dx_out[:, s * strip : (s + 1) * strip] = dx_sum[2 * s : 2 * s + 2, :].astype(jnp.bfloat16)
    for copy in ring + list(crossing.values()) + meta_copies + core_copies + score_copies + dx_copies:
        copy.wait_send()


def weight_kernel(
    x_ref, y_ref, pre_ref, upper_ref, scaled_ref, dx_ref, prob_ref,
    gate_ref, up_ref, down_ref, token_ref, score_ref,
):
    token_ref[...] = dx_ref[...]
    score_ref[...] = prob_ref[...]
    x = x_ref[...]
    gate_ref[0] = lax.dot_general(x, pre_ref[...], TN, preferred_element_type=jnp.float32).astype(jnp.bfloat16)
    up_ref[0] = lax.dot_general(x, upper_ref[...], TN, preferred_element_type=jnp.float32).astype(jnp.bfloat16)
    down_ref[0] = lax.dot_general(scaled_ref[...], y_ref[...], TN, preferred_element_type=jnp.float32).astype(jnp.bfloat16)


def fits(tokens, expert_ids, gate_weight):
    n_fsdp, n_expert, n_dp = (lax.axis_size(a) for a in ("fsdp", "expert", "dp"))
    group_count = expert_ids.shape[0]
    experts = gate_weight.shape[0] * n_expert
    capacity = 2 * group_count // experts
    width, hidden = gate_weight.shape[1:]
    weights = 3 * gate_weight.size * 2
    return (
        tokens.shape[0] == 2
        and n_fsdp % 2 == 0
        and n_fsdp * TILE_ROWS % 128 == 0
        and capacity % 8 == 0
        and group_count <= 128
        and experts * capacity * n_expert * n_dp < 1 << 20
        and n_expert * capacity % 16 == 0
        and n_expert * n_dp * n_fsdp * TILE_ROWS <= 1024
        and gate_weight.shape[0] * n_expert * capacity * n_dp <= 128
        and width % (128 * n_dp) == 0
        and width % 1024 == 0
        and hidden % 256 == 0
        and weights <= 32 * 1024 * 1024
    )


def fused(tokens, cotangent, expert_ids, slot_ids, route_probs, gate_weight, up_weight, down_weight):
    n_fsdp, n_expert, n_dp = (lax.axis_size(a) for a in ("fsdp", "expert", "dp"))
    local_experts, width, hidden = gate_weight.shape
    experts = local_experts * n_expert
    group_count = expert_ids.shape[0]
    capacity = 2 * group_count // experts
    groups = n_expert * n_dp
    quarter, n_z = width // 4, n_fsdp // 2
    per_rep = n_expert * capacity
    per_expert = n_dp * per_rep
    all_rows = local_experts * per_expert
    own_rows = local_experts * per_rep
    half = width // n_dp
    strips = TILE_ROWS // 2
    strip = width // strips
    back = n_expert * n_fsdp - 1
    cross = groups - 1
    message_rows = n_expert * n_fsdp * TILE_ROWS
    bf16, f32 = jnp.bfloat16, jnp.float32
    dma = pltpu.SemaphoreType.DMA
    vmem = pl.BlockSpec(memory_space=pltpu.VMEM)
    hbm = pl.BlockSpec(memory_space=pl.ANY)
    shape = jax.ShapeDtypeStruct
    half_x, half_y, pre, upper, scaled, dx, prob = pl.pallas_call(
        functools.partial(exchange_kernel, n_fsdp, n_expert, n_dp, capacity),
        out_shape=[
            shape((all_rows, half), bf16),
            shape((all_rows, half), bf16),
            shape((all_rows, hidden), bf16),
            shape((all_rows, hidden), bf16),
            shape((all_rows, hidden), bf16),
            shape((2, width), bf16),
            shape((2, 1, 2), f32),
        ],
        in_specs=[vmem] * 5 + [hbm] * 3,
        out_specs=[vmem] * 7,
        scratch_shapes=[
            pltpu.VMEM((TILE_ROWS, quarter), f32),
            pltpu.VMEM((TILE_ROWS, quarter), bf16),
            pltpu.VMEM((8, 128), f32),
            pltpu.VMEM((8, n_fsdp * TILE_ROWS), f32),
            pltpu.VMEM((TILE_ROWS, strip), f32),
            pltpu.VMEM((local_experts, width, hidden), bf16),
            pltpu.VMEM((local_experts, width, hidden), bf16),
            pltpu.VMEM((local_experts, hidden, width), bf16),
            pltpu.VMEM((groups * n_fsdp, TILE_ROWS, quarter), bf16),
            pltpu.VMEM((groups, 8, n_fsdp * TILE_ROWS), f32),
            pltpu.VMEM((all_rows, width), bf16),
            pltpu.VMEM((all_rows, width), bf16),
            pltpu.VMEM((2, all_rows, groups * n_fsdp * TILE_ROWS), f32),
            pltpu.VMEM((all_rows, 128), f32),
            pltpu.VMEM((strips * own_rows, strip), bf16),
            pltpu.VMEM((message_rows, strip), bf16),
            pltpu.VMEM((back, TILE_ROWS, strip), bf16),
            pltpu.VMEM((message_rows, 128), bf16),
            pltpu.VMEM((back, TILE_ROWS, 128), bf16),
            dma((local_experts, 3)),
            dma((2,)),
            dma((n_z,)),
            dma((n_z,)),
            dma((cross, n_z)),
            dma((cross, n_z)),
            dma((cross,)),
            dma((cross,)),
            dma((groups,)),
            dma((groups,)),
            dma((back,)),
            dma((back,)),
            dma((back,)),
            dma((back,)),
        ],
        compiler_params=pltpu.CompilerParams(
            collective_id=0, has_side_effects=True, vmem_limit_bytes=56 * 1024 * 1024
        ),
    )(
        tokens[:, 0, :], cotangent[:, 0, :], expert_ids[:, 0, :].T, slot_ids[:, 0, :].T,
        route_probs[:, 0, :].T, gate_weight, up_weight, down_weight,
    )

    tile = 256
    steps = half // tile
    row_block = pl.BlockSpec((per_expert, tile), lambda k, i: (k, i))
    full_hidden = pl.BlockSpec((per_expert, hidden), lambda k, i: (k, 0))
    hidden_tile = hidden // steps
    dx_block = pl.BlockSpec((2, width), lambda k, i: (0, 0))
    prob_block = pl.BlockSpec((2, 1, 2), lambda k, i: (0, 0, 0))
    grad_gate, grad_up, grad_down, dx, prob = pl.pallas_call(
        weight_kernel,
        grid=(local_experts, steps),
        out_shape=[
            shape((local_experts, half, hidden), bf16),
            shape((local_experts, half, hidden), bf16),
            shape((local_experts, hidden, half), bf16),
            shape((2, width), bf16),
            shape((2, 1, 2), f32),
        ],
        in_specs=[
            row_block,
            pl.BlockSpec((per_expert, half), lambda k, i: (k, 0)),
            full_hidden,
            full_hidden,
            pl.BlockSpec((per_expert, hidden_tile), lambda k, i: (k, i)),
            dx_block,
            prob_block,
        ],
        out_specs=[
            pl.BlockSpec((1, tile, hidden), lambda k, i: (k, i, 0)),
            pl.BlockSpec((1, tile, hidden), lambda k, i: (k, i, 0)),
            pl.BlockSpec((1, hidden_tile, half), lambda k, i: (k, i, 0)),
            dx_block,
            prob_block,
        ],
        compiler_params=pltpu.CompilerParams(
            dimension_semantics=("arbitrary", "arbitrary"), vmem_limit_bytes=60 * 1024 * 1024
        ),
    )(half_x, half_y, pre, upper, scaled, dx, prob)
    token_grad = dx.reshape(2, 1, width)
    return grad_gate, grad_up, grad_down, token_grad, prob


def either_way(tokens, cotangent, expert_ids, slot_ids, route_probs, gate_weight, up_weight, down_weight):
    way = fused if fits(tokens, expert_ids, gate_weight) else shards
    return way(tokens, cotangent, expert_ids, slot_ids, route_probs, gate_weight, up_weight, down_weight)


def route_rows(group_ids, group_slots, local_count, peer_count, capacity):
    kept_slot = group_slots >= 0
    target = (
        group_ids % local_count * (peer_count * capacity)
        + group_ids // local_count * capacity
        + jnp.where(kept_slot, group_slots, 0)
    )
    total_rows = local_count * peer_count * capacity
    row_iota = lax.broadcasted_iota(jnp.int32, (total_rows, group_ids.shape[0]), 0)
    leading = jnp.logical_and(row_iota == target[None, :, 0], kept_slot[None, :, 0])
    trailing = jnp.logical_and(row_iota == target[None, :, 1], kept_slot[None, :, 1])
    return (leading, trailing)


def summed(values):
    return jnp.sum(
        lax.optimization_barrier(values.astype(jnp.bfloat16)).astype(jnp.float32), axis=1
    )


def shards(
    tokens, cotangent, expert_ids, slot_ids, route_probs, gate_weight, up_weight, down_weight
):
    local_experts = gate_weight.shape[0]
    model_width = tokens.shape[2]
    group_count = expert_ids.shape[0]
    peer_count = lax.axis_size("expert")
    capacity = 2 * group_count // (local_experts * peer_count)
    per_expert = peer_count * capacity
    total_rows = local_experts * per_expert
    leading, trailing = route_rows(
        expert_ids[:, 0, :], slot_ids[:, 0, :], local_experts, peer_count, capacity
    )
    either = jnp.logical_or(leading, trailing).astype(jnp.bfloat16)
    prob_pair = route_probs[:, 0, :].astype(jnp.float32)
    prob_rows = jnp.sum(
        jnp.where(leading, prob_pair[None, :, 0], 0.0)
        + jnp.where(trailing, prob_pair[None, :, 1], 0.0),
        axis=1,
    )
    prob_rows = prob_rows.astype(jnp.bfloat16).reshape(local_experts, peer_count, capacity)
    own_x = tokens[:, 0, :]
    own_dy = cotangent[:, 0, :]
    group_x, group_dy = (
        lax.all_gather(own_x, "fsdp", axis=0, tiled=True),
        lax.all_gather(own_dy, "fsdp", axis=0, tiled=True),
    )
    sent_x = (
        jnp.dot(either, group_x, preferred_element_type=jnp.float32)
        .astype(jnp.bfloat16)
        .reshape(local_experts, peer_count, capacity, model_width)
    )
    sent_dy = (
        jnp.dot(either, group_dy, preferred_element_type=jnp.float32)
        .astype(jnp.bfloat16)
        .reshape(local_experts, peer_count, capacity, model_width)
    )
    recv_x, recv_dy, recv_prob = (
        lax.all_to_all(sent_x, "expert", split_axis=1, concat_axis=1, tiled=True),
        lax.all_to_all(sent_dy, "expert", split_axis=1, concat_axis=1, tiled=True),
        lax.all_to_all(prob_rows, "expert", split_axis=1, concat_axis=1, tiled=True),
    )
    rows_x = recv_x.reshape(local_experts, per_expert, model_width)
    rows_dy = recv_dy.reshape(local_experts, per_expert, model_width)
    prob_column = recv_prob.reshape(local_experts, per_expert, 1).astype(jnp.float32)
    gate_value = jnp.einsum("erd,edh->erh", rows_x, gate_weight, preferred_element_type=jnp.float32)
    up_value = jnp.einsum("erd,edh->erh", rows_x, up_weight, preferred_element_type=jnp.float32)
    back_value = jnp.einsum(
        "erd,ehd->erh", rows_dy, down_weight, preferred_element_type=jnp.float32
    )
    sigmoid_gate = jax.nn.sigmoid(gate_value)
    swish_gate = gate_value * sigmoid_gate
    hidden_full = swish_gate * up_value
    hidden = hidden_full.astype(jnp.bfloat16)
    scaled = (prob_column * hidden_full).astype(jnp.bfloat16)
    row_score = jnp.sum(hidden.astype(jnp.float32) * back_value, axis=2)
    back_scaled = prob_column * back_value
    grad_pre = (
        back_scaled * up_value * sigmoid_gate * (1.0 + gate_value * (1.0 - sigmoid_gate))
    ).astype(jnp.bfloat16)
    grad_upper = (back_scaled * swish_gate).astype(jnp.bfloat16)
    slot_dx = jnp.einsum(
        "erh,edh->erd", grad_pre, gate_weight, preferred_element_type=jnp.float32
    ) + jnp.einsum("erh,edh->erd", grad_upper, up_weight, preferred_element_type=jnp.float32)
    replica_count = lax.axis_size("dp")
    far_x, far_dy = (
        lax.all_to_all(rows_x, "dp", split_axis=2, concat_axis=1, tiled=True),
        lax.all_to_all(rows_dy, "dp", split_axis=2, concat_axis=1, tiled=True),
    )
    far_pre, far_upper, far_scaled = (
        lax.all_gather(grad_pre, "dp", axis=1, tiled=True),
        lax.all_gather(grad_upper, "dp", axis=1, tiled=True),
        lax.all_gather(scaled, "dp", axis=1, tiled=True),
    )
    quarter = far_x.shape[2]
    hidden_count = far_pre.shape[2]
    far_x = far_x.reshape(local_experts, replica_count, per_expert, quarter)
    far_dy = far_dy.reshape(local_experts, replica_count, per_expert, quarter)
    far_pre = far_pre.reshape(local_experts, replica_count, per_expert, hidden_count)
    far_upper = far_upper.reshape(local_experts, replica_count, per_expert, hidden_count)
    far_scaled = far_scaled.reshape(local_experts, replica_count, per_expert, hidden_count)
    grad_gate = summed(
        jnp.einsum("esrd,esrh->esdh", far_x, far_pre, preferred_element_type=jnp.float32)
    )
    grad_up = summed(
        jnp.einsum("esrd,esrh->esdh", far_x, far_upper, preferred_element_type=jnp.float32)
    )
    grad_down = summed(
        jnp.einsum("esrh,esrd->eshd", far_scaled, far_dy, preferred_element_type=jnp.float32)
    )
    back_dx, back_score = (
        lax.all_to_all(
            slot_dx.reshape(local_experts, peer_count, capacity, model_width).astype(jnp.bfloat16),
            "expert",
            split_axis=1,
            concat_axis=1,
            tiled=True,
        ).astype(jnp.float32),
        lax.all_to_all(
            row_score.reshape(local_experts, peer_count, capacity).astype(jnp.bfloat16),
            "expert",
            split_axis=1,
            concat_axis=1,
            tiled=True,
        ).astype(jnp.float32),
    )
    flat_dx = back_dx.reshape(total_rows, model_width)
    flat_score = back_score.reshape(total_rows)
    leading_f = leading.astype(jnp.float32)
    trailing_f = trailing.astype(jnp.float32)
    group_dx = lax.dot_general(
        leading_f + trailing_f, flat_dx, (((0,), (0,)), ((), ())), precision=lax.Precision.HIGHEST
    )
    group_prob = jnp.stack(
        [
            jnp.dot(flat_score, leading_f, precision=lax.Precision.HIGHEST),
            jnp.dot(flat_score, trailing_f, precision=lax.Precision.HIGHEST),
        ],
        axis=1,
    )
    token_dx, token_prob = (
        lax.psum_scatter(group_dx, "fsdp", scatter_dimension=0, tiled=True),
        lax.psum_scatter(group_prob, "fsdp", scatter_dimension=0, tiled=True),
    )
    return (
        grad_gate.astype(jnp.bfloat16),
        grad_up.astype(jnp.bfloat16),
        grad_down.astype(jnp.bfloat16),
        token_dx.astype(jnp.bfloat16)[:, None, :],
        token_prob[:, None, :],
    )


def solution(mesh):
    return jax.shard_map(
        either_way,
        mesh=mesh,
        in_specs=(
            P("fsdp", ("expert", "dp"), None),
            P("fsdp", ("expert", "dp"), None),
            P(None, ("expert", "dp"), None),
            P(None, ("expert", "dp"), None),
            P(None, ("expert", "dp"), None),
            P("expert", None, "fsdp"),
            P("expert", None, "fsdp"),
            P("expert", "fsdp", None),
        ),
        out_specs=(
            P("expert", "dp", "fsdp"),
            P("expert", "dp", "fsdp"),
            P("expert", "fsdp", "dp"),
            P("fsdp", ("expert", "dp"), None),
            P("fsdp", ("expert", "dp"), None),
        ),
        check_vma=False,
    )
```
